32 devices in a mesh: gz: 16 (over z, y, x), gy: 2 (over core).
Axes of the slice: x: 2, y: 2, z: 4, core: 2. Of those that a mesh axis runs over, the one named last changes fastest.
Arguments:
- snapshots: float32 [48, 64, 128, 256], P(None, 'gz', 'gy'), may hold values from -6 to 6
- energies: float32 [48], replicated, may hold values from 0.3 to 3
- plane_weight: float32 [64], P('gz'), may hold values from 1 to 10
Outputs:
- modes: float32 [16, 64, 128, 256], P(None, 'gz', 'gy')
- basis: float32 [48, 16], replicated
The draws below stay inside these ranges and needn't reach their ends.
All inputs are finite; a program needn't handle non-finite values.
Results may differ from the reference program's by a relative error of at most 0.0003.
Values sent between devices are 32-bit elements; how exact they have to be, the bound alone decides.
No kernel may reach another device: no remote copies, remote signals or barrier semaphores. Data moves between devices by JAX's collectives and lax.ppermute only.
A program may use at most 128 MiB of HBM per device.

```python
import math
import jax
import jax.numpy as jnp
from jax import lax

S = 48
MODES = 16
ITERS = 6
NXF = 256
NY = 128
NZ = 64


def block_levels(own_key, dims, pieces, low, high):
    gain = 1.0
    for position, shards_of in pieces:
        steps = jax.random.uniform(jax.random.fold_in(jax.random.fold_in(own_key, 6), position), (shards_of,), jnp.float32, low / len(pieces), high / len(pieces))
        gain = gain * jnp.repeat(jnp.exp(steps), dims[position] // shards_of).reshape((-1,) + (1,) * (len(dims) - 1 - position))
    return gain


def bell_draw(rng, dims, scale, limit, split=(), kind=jnp.bfloat16):
    loudness = block_levels(rng, dims, split, -0.22, 0.18) if split else 1.0
    entries = jax.random.normal(rng, dims, jnp.float32) * scale * loudness
    return jnp.minimum(jnp.maximum(entries, -limit), limit).astype(kind)


def setup_inputs(seed: int = 0) -> dict:
    key_list = jax.random.split(jax.random.key(seed), 4)
    return {
        "snapshots": bell_draw(key_list[0], (S, NZ, NY, NXF), 1.0, 6.0, ((1, 16), (2, 2)), jnp.float32),
        "energies": jnp.clip(jnp.exp(jax.random.uniform(key_list[1], (S,), jnp.float32, math.log(0.3), math.log(3.0))), 0.3, 3.0),
        "plane_weight": jnp.clip(jnp.exp(math.log(10.0) - 2.3025851 * jax.random.uniform(key_list[2], (NZ,), jnp.float32) ** block_levels(key_list[2], (NZ,), ((0, 16),), -0.2, 0.2)), 1.0, 10.0),
    }


def reference(snapshots, energies, plane_weight):
    scaled = snapshots * energies[:, None, None, None]
    filtered = 0.25 * jnp.roll(scaled, 1, axis=1) + 0.5 * scaled + 0.25 * jnp.roll(scaled, -1, axis=1)
    total = filtered.shape[1] * filtered.shape[2] * filtered.shape[3]

    def add_plane(index, gram):
        plane = lax.dynamic_index_in_dim(filtered, index, 1, keepdims=False).reshape(S, -1)
        weight = lax.dynamic_index_in_dim(plane_weight, index, 0, keepdims=False)
        return gram + jnp.dot(plane * weight, plane.T, precision=lax.Precision.HIGHEST)
    gram = lax.fori_loop(0, NZ, add_plane, jnp.zeros((S, S), jnp.float32)) / total
    basis = jnp.eye(S, dtype=jnp.float32)[:, :MODES]
    for step in range(ITERS):
        image = jnp.dot(gram, basis, precision=lax.Precision.HIGHEST)
        factor = jnp.linalg.cholesky(jnp.dot(image.T, image, precision=lax.Precision.HIGHEST))
        basis = jax.scipy.linalg.solve_triangular(factor, image.T, lower=True).T
    raw = jnp.dot(basis.T, filtered.reshape(S, -1), precision=lax.Precision.HIGHEST)
    raw = raw.reshape(MODES, NZ, NY, NXF)
    norms = lax.optimization_barrier(jnp.sum(raw * raw * plane_weight[None, :, None, None], axis=(1, 2, 3))) / total
    modes = raw / jnp.sqrt(norms)[:, None, None, None]
    return (modes, basis)
```

```python
import jax
import jax.numpy as jnp
from jax import lax
from jax.experimental import pallas as pl
from jax.experimental.pallas import tpu as pltpu
from jax.sharding import PartitionSpec as P

MODES = 16
ITERS = 6
CHUNKS = 4
SUB = 8
F32 = jnp.float32
BF16 = jnp.bfloat16
HIGHEST = lax.Precision.HIGHEST
LAST = (((1,), (1,)), ((), ()))
INNER = (((1,), (0,)), ((), ()))


def mm(a, b, dims=INNER, precision=None):
    return lax.dot_general(a, b, dims, precision=precision, preferred_element_type=F32)


def split(value):
    high = value.astype(BF16)
    return high, (value - high.astype(F32)).astype(BF16)


def selector(shape, group_dim):
    grouped = lax.broadcasted_iota(jnp.int32, shape, group_dim) // SUB
    other = lax.broadcasted_iota(jnp.int32, shape, 1 - group_dim)
    return (grouped == other).astype(F32)


def same_row(shape):
    a = lax.broadcasted_iota(jnp.int32, shape, 0) % SUB
    b = lax.broadcasted_iota(jnp.int32, shape, 1) % SUB
    return a == b


def accumulate(hh_ref, hl_ref, field, weight, first):
    count, sub, width = field.shape
    flat = field.reshape(count * sub, width) * jnp.sqrt(jnp.full((1, width), weight, F32))
    high, low = split(flat)
    hh, hl = mm(high, high, LAST), mm(high, low, LAST)
    if first:
        hh_ref[...] = hh
        hl_ref[...] = hl
    else:
        hh_ref[...] += hh
        hl_ref[...] += hl


def finish(gram_ref, hh_ref, hl_ref):
    total = hh_ref[...] + 2.0 * hl_ref[...]
    total = jnp.where(same_row(total.shape), total, 0.0)
    count = gram_ref.shape[0]
    pick = selector((count, total.shape[0]), 1)
    half = mm(pick, total, INNER, HIGHEST)
    gram_ref[...] = mm(half, pick, LAST, HIGHEST)


def interior_kernel(weight_ref, snap_ref, field_ref, gram_ref, hh_ref, hl_ref):
    planes = snap_ref.shape[1]
    step = pl.program_id(0)

    @pl.when(step == 0)
    def _():
        hh_ref[...] = jnp.zeros(hh_ref.shape, F32)
        hl_ref[...] = jnp.zeros(hl_ref.shape, F32)

    field_ref[:, 0] = 0.5 * snap_ref[:, 0] + 0.25 * snap_ref[:, 1]
    field_ref[:, planes - 1] = 0.25 * snap_ref[:, planes - 2] + 0.5 * snap_ref[:, planes - 1]
    for z in range(1, planes - 1):
        field = 0.25 * (snap_ref[:, z - 1] + snap_ref[:, z + 1]) + 0.5 * snap_ref[:, z]
        field_ref[:, z] = field
        accumulate(hh_ref, hl_ref, field, weight_ref[z], False)

    @pl.when(step == pl.num_programs(0) - 1)
    def _():
        finish(gram_ref, hh_ref, hl_ref)


def interior(snapshots, weight):
    count, planes, rows, width = snapshots.shape
    block = pl.BlockSpec((count, planes, SUB, width), lambda i: (0, 0, i, 0))
    return pl.pallas_call(
        interior_kernel,
        grid=(rows // SUB,),
        in_specs=[pl.BlockSpec(memory_space=pltpu.SMEM), block],
        out_specs=[block, pl.BlockSpec((count, count), lambda i: (0, 0))],
        out_shape=[
            jax.ShapeDtypeStruct(snapshots.shape, F32),
            jax.ShapeDtypeStruct((count, count), F32),
        ],
        scratch_shapes=[pltpu.VMEM((count * SUB, count * SUB), F32)] * 2,
        compiler_params=pltpu.CompilerParams(dimension_semantics=("arbitrary",)),
        name="interior",
    )(weight, snapshots)


def edge_kernel(weight_ref, low_ref, high_ref, bottom_ref, top_ref, prior_ref,
                edge_ref, gram_ref, hh_ref, hl_ref):
    planes = weight_ref.shape[0]
    step = pl.program_id(0)

    @pl.when(step == 0)
    def _():
        hh_ref[...] = jnp.zeros(hh_ref.shape, F32)
        hl_ref[...] = jnp.zeros(hl_ref.shape, F32)

    bottom = bottom_ref[:, 0] + 0.25 * low_ref[...]
    top = top_ref[:, 0] + 0.25 * high_ref[...]
    edge_ref[:, 0] = bottom
    edge_ref[:, 1] = top
    accumulate(hh_ref, hl_ref, bottom, weight_ref[0], False)
    accumulate(hh_ref, hl_ref, top, weight_ref[planes - 1], False)

    @pl.when(step == pl.num_programs(0) - 1)
    def _():
        finish(gram_ref, hh_ref, hl_ref)
        gram_ref[...] += prior_ref[...]


def edge(weight, low, high, field, prior, chunk):
    count, rows, width = low.shape
    planes = field.shape[1]
    base = chunk * (rows // SUB)
    halo = pl.BlockSpec((count, SUB, width), lambda i: (0, i, 0))
    whole = pl.BlockSpec((count, count), lambda i: (0, 0))
    return pl.pallas_call(
        edge_kernel,
        grid=(rows // SUB,),
        in_specs=[
            pl.BlockSpec(memory_space=pltpu.SMEM),
            halo,
            halo,
            pl.BlockSpec((count, 1, SUB, width), lambda i: (0, 0, base + i, 0)),
            pl.BlockSpec((count, 1, SUB, width), lambda i: (0, planes - 1, base + i, 0)),
            whole,
        ],
        out_specs=[pl.BlockSpec((count, 2, SUB, width), lambda i: (0, 0, i, 0)), whole],
        out_shape=[
            jax.ShapeDtypeStruct((count, 2, rows, width), F32),
            jax.ShapeDtypeStruct((count, count), F32),
        ],
        scratch_shapes=[pltpu.VMEM((count * SUB, count * SUB), F32)] * 2,
        compiler_params=pltpu.CompilerParams(dimension_semantics=("arbitrary",)),
        name="edge",
    )(weight, low, high, field, field, prior)


def orthonormal(image):
    modes = image.shape[0]
    square = mm(image, image, LAST, HIGHEST)
    columns = [jnp.broadcast_to(square[:, j:j + 1], (modes, 128)) for j in range(modes)]
    row = lax.broadcasted_iota(jnp.int32, (modes, 1), 0)
    lanes = image.shape[1]
    for j in range(modes):
        scale = lax.rsqrt(columns[j][j:j + 1, :])
        left = columns[j] * scale
        pivot = image[j:j + 1, :] * scale[:, :lanes]
        lower = jnp.where(row > j, left, 0.0)
        image = jnp.where(row == j, pivot, image - lower[:, :lanes] * pivot)
        for t in range(j + 1, modes):
            columns[t] = columns[t] - left * (columns[t][j:j + 1, :] * scale)
    return image


def modes_kernel(total, gram_ref, outer_ref, energy_ref, eye_ref, field_hbm, *rest):
    edges_hbm = rest[:CHUNKS]
    out_hbm, basis_ref, field_ref, stage_ref, in_sems, out_sems = rest[CHUNKS:]
    count, planes, rows, width = field_ref.shape
    modes = basis_ref.shape[0]
    part = rows // CHUNKS
    loads = []
    for c in range(CHUNKS):
        ys = pl.ds(c * part, part)
        loads.append([
            pltpu.make_async_copy(edges_hbm[c].at[:, pl.ds(0, 1)],
                                  field_ref.at[:, pl.ds(0, 1), ys], in_sems.at[c, 0]),
            pltpu.make_async_copy(field_hbm.at[:, pl.ds(1, planes - 2), ys],
                                  field_ref.at[:, pl.ds(1, planes - 2), ys], in_sems.at[c, 1]),
            pltpu.make_async_copy(edges_hbm[c].at[:, pl.ds(1, 1)],
                                  field_ref.at[:, pl.ds(planes - 1, 1), ys], in_sems.at[c, 2]),
        ])
    for group in loads:
        for copy in group:
            copy.start()

    gram = gram_ref[...]
    gram = (0.5 / total) * (gram + gram.T) * outer_ref[...]
    basis = eye_ref[...]
    for _ in range(ITERS):
        basis = orthonormal(mm(basis, gram, INNER, HIGHEST))
    basis_ref[...] = basis
    norms = jnp.sum(basis * mm(basis, gram, INNER, HIGHEST), axis=1, keepdims=True)
    high, low = split(basis * energy_ref[...] / jnp.sqrt(norms))
    left = selector((modes * SUB, modes), 0).astype(BF16)
    right = selector((count, count * SUB), 1).astype(BF16)
    mask = same_row((modes * SUB, count * SUB))

    def spread(value):
        wide = mm(mm(left, value).astype(BF16), right)
        return jnp.where(mask, wide, 0.0).astype(BF16)

    high, low = spread(high), spread(low)
    stores = []
    for c in range(CHUNKS):
        for copy in loads[c]:
            copy.wait()
        for z in range(planes):
            for g in range(part // SUB):
                ys = pl.ds(c * part + g * SUB, SUB)
                block = field_ref[:, z, ys, :].reshape(count * SUB, width)
                f_high, f_low = split(block)
                result = mm(high, f_high) + (mm(high, f_low) + mm(low, f_high))
                stage_ref[:, z, ys, :] = result.reshape(modes, SUB, width)
        ys = pl.ds(c * part, part)
        copy = pltpu.make_async_copy(stage_ref.at[:, :, ys], out_hbm.at[:, :, ys], out_sems.at[c])
        copy.start()
        stores.append(copy)
    for copy in stores:
        copy.wait()


def project(gram, energies, field, edges, total):
    count, planes, rows, width = field.shape
    whole = pl.BlockSpec(memory_space=pltpu.VMEM)
    anywhere = pl.BlockSpec(memory_space=pl.ANY)
    outer = energies[:, None] * energies[None, :]
    eye = jnp.eye(count, dtype=F32)[:MODES]
    return pl.pallas_call(
        lambda *refs: modes_kernel(total, *refs),
        in_specs=[whole, whole, whole, whole, anywhere] + [anywhere] * CHUNKS,
        out_specs=[anywhere, whole],
        out_shape=[
            jax.ShapeDtypeStruct((MODES, planes, rows, width), F32),
            jax.ShapeDtypeStruct((MODES, count), F32),
        ],
        scratch_shapes=[
            pltpu.VMEM((count, planes, rows, width), F32),
            pltpu.VMEM((MODES, planes, rows, width), F32),
            pltpu.SemaphoreType.DMA((CHUNKS, 3)),
            pltpu.SemaphoreType.DMA((CHUNKS,)),
        ],
        compiler_params=pltpu.CompilerParams(vmem_limit_bytes=48 * 2**20),
        name="project",
    )(gram, outer, energies[None, :], eye, field, *edges)


def sum_over_all(value, axes):
    devices = lax.axis_size(axes)
    if devices & (devices - 1):
        return lax.psum(value, axes)
    bit = 1
    while bit < devices:
        value = value + lax.ppermute(value, axes, [(i, i ^ bit) for i in range(devices)])
        bit *= 2
    return value


def local(snapshots, energies, plane_weight):
    count, planes, rows, width = snapshots.shape
    ring = lax.axis_size("gz")
    total = planes * ring * rows * lax.axis_size("gy") * width
    forward = [(i, (i + 1) % ring) for i in range(ring)]
    backward = [(target, source) for source, target in forward]
    part = rows // CHUNKS
    halos = []
    for c in range(CHUNKS):
        ys = slice(c * part, (c + 1) * part)
        low = lax.ppermute(snapshots[:, planes - 1, ys], "gz", forward)
        high = lax.ppermute(snapshots[:, 0, ys], "gz", backward)
        halos.append((low, high))
    field, gram = interior(snapshots, plane_weight)
    edges = []
    for c, (low, high) in enumerate(halos):
        piece, gram = edge(plane_weight, low, high, field, gram, c)
        edges.append(piece)
    gram = sum_over_all(gram, ("gz", "gy"))
    modes, basis = project(gram, energies, field, edges, total)
    return (modes, basis.T)


def solution(mesh):
    placed = (P(None, "gz", "gy", None), P(), P("gz"))
    return jax.shard_map(
        local,
        mesh=mesh,
        in_specs=placed,
        out_specs=(P(None, "gz", "gy", None), P()),
        check_vma=False,
    )
```

```python
import jax
import jax.numpy as jnp
from jax import lax
from jax.experimental import pallas as pl
from jax.experimental.pallas import tpu as pltpu
from jax.sharding import PartitionSpec as P

MODES = 16
ITERS = 6
SHARES = (2, 3, 2, 1)
CHUNKS = len(SHARES)
SUB = 8
F32 = jnp.float32
BF16 = jnp.bfloat16
HIGHEST = lax.Precision.HIGHEST
LAST = (((1,), (1,)), ((), ()))
INNER = (((1,), (0,)), ((), ()))


def bounds(rows):
    groups, weight, done, result = rows // SUB, sum(SHARES), 0, []
    for c in range(CHUNKS):
        end = groups * sum(SHARES[:c + 1]) // weight
        result.append((done * SUB, (end - done) * SUB))
        done = end
    return result


def mm(a, b, dims=INNER, precision=None):
    return lax.dot_general(a, b, dims, precision=precision, preferred_element_type=F32)


def split(value):
    high = value.astype(BF16)
    return high, (value - high.astype(F32)).astype(BF16)


def selector(shape, group_dim):
    grouped = lax.broadcasted_iota(jnp.int32, shape, group_dim) // SUB
    other = lax.broadcasted_iota(jnp.int32, shape, 1 - group_dim)
    return (grouped == other).astype(F32)


def same_row(shape):
    a = lax.broadcasted_iota(jnp.int32, shape, 0) % SUB
    b = lax.broadcasted_iota(jnp.int32, shape, 1) % SUB
    return a == b


def accumulate(hh_ref, hl_ref, field, weight, first):
    count, sub, width = field.shape
    flat = field.reshape(count * sub, width) * jnp.sqrt(jnp.full((1, width), weight, F32))
    high, low = split(flat)
    hh, hl = mm(high, high, LAST), mm(high, low, LAST)
    if first:
        hh_ref[...] = hh
        hl_ref[...] = hl
    else:
        hh_ref[...] += hh
        hl_ref[...] += hl


def finish(gram_ref, hh_ref, hl_ref):
    total = hh_ref[...] + 2.0 * hl_ref[...]
    total = jnp.where(same_row(total.shape), total, 0.0)
    count = gram_ref.shape[0]
    pick = selector((count, total.shape[0]), 1).astype(BF16)
    first = total.astype(BF16)
    second, third = split(total - first.astype(F32))
    half = mm(pick, first) + (mm(pick, second) + mm(pick, third))
    first = half.astype(BF16)
    second, third = split(half - first.astype(F32))
    gram_ref[...] = mm(first, pick, LAST) + (mm(second, pick, LAST) + mm(third, pick, LAST))


def interior_kernel(weight_ref, snap_ref, field_ref, gram_ref, hh_ref, hl_ref):
    planes = snap_ref.shape[1]
    step = pl.program_id(0)

    @pl.when(step == 0)
    def _():
        hh_ref[...] = jnp.zeros(hh_ref.shape, F32)
        hl_ref[...] = jnp.zeros(hl_ref.shape, F32)

    field_ref[:, 0] = 0.5 * snap_ref[:, 0] + 0.25 * snap_ref[:, 1]
    field_ref[:, planes - 1] = 0.25 * snap_ref[:, planes - 2] + 0.5 * snap_ref[:, planes - 1]
    for z in range(1, planes - 1):
        field = 0.25 * (snap_ref[:, z - 1] + snap_ref[:, z + 1]) + 0.5 * snap_ref[:, z]
        field_ref[:, z] = field
        accumulate(hh_ref, hl_ref, field, weight_ref[z], False)

    @pl.when(step == pl.num_programs(0) - 1)
    def _():
        finish(gram_ref, hh_ref, hl_ref)


def interior(snapshots, weight):
    count, planes, rows, width = snapshots.shape
    block = pl.BlockSpec((count, planes, SUB, width), lambda i: (0, 0, i, 0))
    return pl.pallas_call(
        interior_kernel,
        grid=(rows // SUB,),
        in_specs=[pl.BlockSpec(memory_space=pltpu.SMEM), block],
        out_specs=[block, pl.BlockSpec((count, count), lambda i: (0, 0))],
        out_shape=[
            jax.ShapeDtypeStruct(snapshots.shape, F32),
            jax.ShapeDtypeStruct((count, count), F32),
        ],
        scratch_shapes=[pltpu.VMEM((count * SUB, count * SUB), F32)] * 2,
        compiler_params=pltpu.CompilerParams(
            dimension_semantics=("arbitrary",), vmem_limit_bytes=32 * 2**20
        ),
        name="interior",
    )(weight, snapshots)


def edge_kernel(weight_ref, low_ref, high_ref, bottom_ref, top_ref, prior_ref,
                edge_ref, gram_ref, hh_ref, hl_ref):
    planes = weight_ref.shape[0]
    step = pl.program_id(0)

    @pl.when(step == 0)
    def _():
        hh_ref[...] = jnp.zeros(hh_ref.shape, F32)
        hl_ref[...] = jnp.zeros(hl_ref.shape, F32)

    ys = pl.ds(step * SUB, SUB)
    bottom = bottom_ref[:, 0] + 0.25 * low_ref[:, ys]
    top = top_ref[:, 0] + 0.25 * high_ref[:, ys]
    edge_ref[:, 0] = bottom
    edge_ref[:, 1] = top
    accumulate(hh_ref, hl_ref, bottom, weight_ref[0], False)
    accumulate(hh_ref, hl_ref, top, weight_ref[planes - 1], False)

    @pl.when(step == pl.num_programs(0) - 1)
    def _():
        finish(gram_ref, hh_ref, hl_ref)
        gram_ref[...] += prior_ref[...]


def edge(weight, low, high, field, prior, start):
    count, rows, width = low.shape
    planes = field.shape[1]
    base = start // SUB
    halo = pl.BlockSpec(memory_space=pltpu.VMEM)
    whole = pl.BlockSpec((count, count), lambda i: (0, 0))
    return pl.pallas_call(
        edge_kernel,
        grid=(rows // SUB,),
        in_specs=[
            pl.BlockSpec(memory_space=pltpu.SMEM),
            halo,
            halo,
            pl.BlockSpec((count, 1, SUB, width), lambda i: (0, 0, base + i, 0)),
            pl.BlockSpec((count, 1, SUB, width), lambda i: (0, planes - 1, base + i, 0)),
            whole,
        ],
        out_specs=[pl.BlockSpec((count, 2, SUB, width), lambda i: (0, 0, i, 0)), whole],
        out_shape=[
            jax.ShapeDtypeStruct((count, 2, rows, width), F32),
            jax.ShapeDtypeStruct((count, count), F32),
        ],
        scratch_shapes=[pltpu.VMEM((count * SUB, count * SUB), F32)] * 2,
        compiler_params=pltpu.CompilerParams(
            dimension_semantics=("arbitrary",), vmem_limit_bytes=24 * 2**20
        ),
        name="edge",
    )(weight, low, high, field, field, prior)


def orthonormal(image):
    modes = image.shape[0]
    square = mm(image, image, LAST, HIGHEST)
    columns = [jnp.broadcast_to(square[:, j:j + 1], (modes, 128)) for j in range(modes)]
    row = lax.broadcasted_iota(jnp.int32, (modes, 1), 0)
    lanes = image.shape[1]
    for j in range(modes):
        scale = lax.rsqrt(columns[j][j:j + 1, :])
        left = columns[j] * scale
        pivot = image[j:j + 1, :] * scale[:, :lanes]
        lower = jnp.where(row > j, left, 0.0)
        image = jnp.where(row == j, pivot, image - lower[:, :lanes] * pivot)
        for t in range(j + 1, modes):
            columns[t] = columns[t] - left * (columns[t][j:j + 1, :] * scale)
    return image


def modes_kernel(total, gram_ref, outer_ref, energy_ref, eye_ref, field_ref, *rest):
    edge_refs = rest[:CHUNKS]
    out_hbm, basis_ref, stage_ref, out_sems = rest[CHUNKS:]
    count, planes, rows, width = field_ref.shape
    modes = basis_ref.shape[0]
    gram = gram_ref[...]
    gram = (0.5 / total) * (gram + gram.T) * outer_ref[...]
    basis = eye_ref[...]
    for _ in range(ITERS):
        basis = orthonormal(mm(basis, gram, INNER, HIGHEST))
    basis_ref[...] = basis
    norms = jnp.sum(basis * mm(basis, gram, INNER, HIGHEST), axis=1, keepdims=True)
    high, low = split(basis * energy_ref[...] / jnp.sqrt(norms))
    left = selector((modes * SUB, modes), 0).astype(BF16)
    right = selector((count, count * SUB), 1).astype(BF16)
    mask = same_row((modes * SUB, count * SUB))

    def spread(value):
        wide = mm(mm(left, value).astype(BF16), right)
        return jnp.where(mask, wide, 0.0).astype(BF16)

    high, low = spread(high), spread(low)
    stores = []
    for c, (start, part) in enumerate(bounds(rows)):
        for z in range(planes):
            for g in range(part // SUB):
                ys = pl.ds(start + g * SUB, SUB)
                if z in (0, planes - 1):
                    block = edge_refs[c][:, min(z, 1), pl.ds(g * SUB, SUB), :]
                else:
                    block = field_ref[:, z, ys, :]
                f_high, f_low = split(block.reshape(count * SUB, width))
                result = mm(high, f_high) + (mm(high, f_low) + mm(low, f_high))
                stage_ref[:, z, ys, :] = result.reshape(modes, SUB, width)
        ys = pl.ds(start, part)
        copy = pltpu.make_async_copy(stage_ref.at[:, :, ys], out_hbm.at[:, :, ys], out_sems.at[c])
        copy.start()
        stores.append(copy)
    for copy in stores:
        copy.wait()


def project(gram, energies, field, edges, total):
    count, planes, rows, width = field.shape
    whole = pl.BlockSpec(memory_space=pltpu.VMEM)
    anywhere = pl.BlockSpec(memory_space=pl.ANY)
    outer = energies[:, None] * energies[None, :]
    eye = jnp.eye(count, dtype=F32)[:MODES]
    return pl.pallas_call(
        lambda *refs: modes_kernel(total, *refs),
        in_specs=[whole] * (5 + CHUNKS),
        out_specs=[anywhere, whole],
        out_shape=[
            jax.ShapeDtypeStruct((MODES, planes, rows, width), F32),
            jax.ShapeDtypeStruct((MODES, count), F32),
        ],
        scratch_shapes=[
            pltpu.VMEM((MODES, planes, rows, width), F32),
            pltpu.SemaphoreType.DMA((CHUNKS,)),
        ],
        compiler_params=pltpu.CompilerParams(vmem_limit_bytes=32 * 2**20),
        name="project",
    )(gram, outer, energies[None, :], eye, field, *edges)


def sum_over_all(value, axes):
    devices = lax.axis_size(axes)
    if devices & (devices - 1):
        return lax.psum(value, axes)
    bit = 1
    while bit < devices:
        value = value + lax.ppermute(value, axes, [(i, i ^ bit) for i in range(devices)])
        bit *= 2
    return value


def local(snapshots, energies, plane_weight):
    count, planes, rows, width = snapshots.shape
    ring = lax.axis_size("gz")
    total = planes * ring * rows * lax.axis_size("gy") * width
    forward = [(i, (i + 1) % ring) for i in range(ring)]
    backward = [(target, source) for source, target in forward]
    chunks = bounds(rows)

    def exchange(source, start, part):
        low, high = source[:, planes - 1, start:start + part], source[:, 0, start:start + part]
        return lax.ppermute(low, "gz", forward), lax.ppermute(high, "gz", backward)

    halos = [exchange(snapshots, *chunk) for chunk in chunks]
    source, first = lax.optimization_barrier((snapshots, halos[0]))
    halos[0] = first
    field, gram = interior(source, plane_weight)
    edges = []
    for (low, high), (start, _) in zip(halos, chunks):
        piece, gram = edge(plane_weight, low, high, field, gram, start)
        edges.append(piece)
    gram = sum_over_all(gram, ("gz", "gy"))
    modes, basis = project(gram, energies, field, edges, total)
    return (modes, basis.T)


def solution(mesh):
    placed = (P(None, "gz", "gy", None), P(), P("gz"))
    return jax.shard_map(
        local,
        mesh=mesh,
        in_specs=placed,
        out_specs=(P(None, "gz", "gy", None), P()),
        check_vma=False,
    )
```
